32 devices in a mesh: corpus: 16 (over z, y, x), batch: 2 (over core).
Axes of the slice: x: 2, y: 2, z: 4, core: 2. Of those that a mesh axis runs over, the one named last changes fastest.
Arguments:
- queries: float32 [128, 1024], P(('corpus', 'batch')), may hold values from -6.25 to 6.25, as said below
- codes: int32 [98304, 32], P('corpus'), may hold values from -2147483648 to 2147483647
- quant_rows: bfloat16 [98304, 1024], P('corpus'), may hold values from -127 to 127, as said below
- row_scale: float32 [98304], P('corpus'), may hold values from 0.0005 to 0.002
- candidates: int32 [128, 40], P(('corpus', 'batch')), may hold values from 0 to 98303
- shortlist: int32 [128], P(('corpus', 'batch')), may hold values from 1 to 40
- edges: int32 [17], replicated, may hold values from 464 to 563, as said below
Outputs:
- hist: float32 [128, 16], P(('corpus', 'batch'))
- scores: float32 [128, 40], P(('corpus', 'batch'))
The draws below stay inside these ranges and needn't reach their ends.
Inputs may be any that keep to these rules, and one draw needn't show every extreme that they name: `queries`: no entry lies within 0.25 of zero. `quant_rows`: whole numbers. `edges`: strictly increasing.
All inputs are finite; a program needn't handle non-finite values.
Results may differ from the reference program's by a relative error of at most 0.0003.
Values sent between devices are 32-bit elements; how exact they have to be, the bound alone decides.
No kernel may reach another device: no remote copies, remote signals or barrier semaphores. Data moves between devices by JAX's collectives and lax.ppermute only.
A program may use at most 64 MiB of HBM per device.

```python
import math
import jax
import jax.numpy as jnp
import numpy as np
from jax import lax

D = 1024
WORDS = 32
QUERIES = 128
ROWS_DEV = 6144
TOTAL_ROWS = 98304
CAND = 40
NBINS = 16
N_CORPUS = 16


def centers(key):
    return jax.random.randint(jax.random.fold_in(key, 101), (16, D), 0, 2).astype(jnp.int32)


def draw_queries(key, part):
    pattern = centers(key)
    member = jax.random.randint(jax.random.fold_in(key, 102), (QUERIES,), 0, 16)
    flip_level = jax.random.randint(jax.random.fold_in(key, 103), (QUERIES, 1), 0, 48)
    flipped = (jax.random.randint(jax.random.fold_in(key, 104), (QUERIES, D), 0, 1024) < flip_level).astype(jnp.int32)
    bits = jnp.bitwise_xor(pattern[member], flipped)
    sign = (2 * bits - 1).astype(jnp.float32)
    normal_part = jax.random.normal(jax.random.fold_in(key, 105), (QUERIES, D), jnp.float32)
    magnitude = 0.25 + jnp.minimum(jnp.abs(normal_part), 6.0)
    return sign * magnitude


def draw_codes(key, part):
    groups = 16
    pattern = centers(key)
    region = jnp.arange(TOTAL_ROWS, dtype=jnp.int32) * groups // TOTAL_ROWS
    member = (region + jax.random.randint(jax.random.fold_in(key, 106), (TOTAL_ROWS,), 0, 2)) % groups
    factor = max(1, 32 // math.isqrt(D))
    level = 512 - jax.random.randint(jax.random.fold_in(key, 107), (groups,), 12, 37) * factor
    chance = level[member] + jax.random.randint(jax.random.fold_in(key, 108), (TOTAL_ROWS,), -16, 17) * factor
    block = math.gcd(TOTAL_ROWS, 2048)
    shifts = jnp.arange(32, dtype=jnp.int32)
    noise_key = jax.random.fold_in(key, 109)

    def one_block(number):
        start = number * block
        own = lax.dynamic_slice_in_dim(member, start, block, 0)
        odds = lax.dynamic_slice_in_dim(chance, start, block, 0)
        noise = (jax.random.randint(jax.random.fold_in(noise_key, number), (block, D), 0, 1024) < odds[:, None]).astype(jnp.int32)
        bits = jnp.bitwise_xor(pattern[own], noise).reshape(block, D // 32, 32)
        return jnp.sum(jnp.left_shift(bits, shifts), axis=2).astype(jnp.int32)
    whole = lax.map(one_block, jnp.arange(TOTAL_ROWS // block, dtype=jnp.int32))
    return whole.reshape(TOTAL_ROWS, D // 32)


def draw_quant_rows(key, part):
    whole = jax.random.randint(key, (TOTAL_ROWS, D), -127, 128)
    return whole.astype(jnp.float32).astype(jnp.bfloat16)


def draw_edges(key, part):
    spacing = max(2, 3 * D // 512)
    jitter = jax.random.randint(key, (NBINS + 1,), 0, spacing // 2 + 1)
    slots = jnp.arange(NBINS + 1, dtype=jnp.int32)
    jitter = jnp.where(slots == 0, 0, jnp.where(slots == NBINS, spacing // 2, jitter))
    start = D // 2 - spacing * (NBINS // 2)
    return (start + spacing * slots + jitter).astype(jnp.int32)


def set_ends(array, stream_key, least, high):
    extent = array.shape
    index_at = [jax.random.randint(jax.random.fold_in(stream_key, axis), (), 0, extent[axis]) for axis in range(len(extent))]
    array = array.at[tuple(index_at)].set(least)
    longest = extent.index(max(extent))
    index_at[longest] = (index_at[longest] + 1) % extent[longest]
    return array.at[tuple(index_at)].set(high)


def levels(stream_key, dims, cuts, low, largest):
    def one(position, shards_of):
        steps = jax.random.uniform(jax.random.fold_in(jax.random.fold_in(stream_key, 6), position), (shards_of,), jnp.float32, low / len(cuts), largest / len(cuts))
        return jnp.repeat(jnp.exp(steps), dims[position] // shards_of).reshape((-1,) + (1,) * (len(dims) - position - 1))

    loudness = one(*cuts[0])
    for cut in cuts[1:]:
        loudness = loudness * one(*cut)
    return loudness


def skewed_wide(key, extent, number_of, lean):
    loads = [min(1 << octave, number_of + 1 - (1 << octave)) * (1 << 20) // math.isqrt((1 << octave) ** lean) + 1 for octave in range((number_of + 1).bit_length()) if 1 << octave <= number_of]
    width = 1 + sum(loads) // (1 << 30)
    table = np.cumsum(np.array([max(1, weight // width) for weight in loads]))
    ticket = jax.random.randint(jax.random.fold_in(key, 1), extent, 0, int(table[len(loads) - 1]))
    start = jnp.left_shift(1, jnp.searchsorted(jnp.asarray(table, jnp.int32), ticket, side="right").astype(jnp.int32))
    standing = start - 1 + jax.random.randint(jax.random.fold_in(key, 4), extent, 0, 1 << 30) % jnp.minimum(start, number_of + 1 - start)
    return jax.random.permutation(jax.random.fold_in(key, 2), number_of)[standing].astype(jnp.int32)


def setup_inputs(seed: int = 0) -> dict:
    splits = jax.random.split(jax.random.key(seed), 8)
    queries = draw_queries(jax.random.fold_in(splits[7], 71), 0)
    codes = draw_codes(jax.random.fold_in(splits[7], 71), 0)
    quant_rows = draw_quant_rows(jax.random.fold_in(splits[7], 71), 0)
    row_scale = jnp.clip(jnp.exp(math.log(0.002) - 1.3862944 * jax.random.uniform(splits[3], (TOTAL_ROWS,), jnp.float32) ** levels(splits[3], (TOTAL_ROWS,), ((0, 16),), -0.2, 0.2)), 0.0005, 0.002)
    candidates = set_ends(skewed_wide(splits[4], (QUERIES, CAND), TOTAL_ROWS, 2), jax.random.fold_in(splits[4], 3), 0, TOTAL_ROWS - 1).astype(jnp.int32)
    shortlist = set_ends(jax.random.randint(splits[5], (QUERIES,), 1, CAND + 1), jax.random.fold_in(splits[5], 1), 1, CAND).astype(jnp.int32)
    edges = draw_edges(jax.random.fold_in(splits[7], 71), 0)
    return dict(queries=queries, codes=codes, quant_rows=quant_rows, row_scale=row_scale, candidates=candidates, shortlist=shortlist, edges=edges)


def unpack(words):
    bits = jnp.right_shift(words[..., None], jnp.arange(32, dtype=jnp.int32)) & 1
    signed = (2 * bits - 1).reshape(words.shape[:-1] + (words.shape[-1] * 32,))
    return signed.astype(jnp.bfloat16)


def reference(queries, codes, quant_rows, row_scale, candidates, shortlist, edges):
    signs = jnp.where(queries >= 0, 1.0, -1.0).astype(jnp.bfloat16)
    limits = edges.astype(jnp.float32)
    blocks = codes.reshape(N_CORPUS, ROWS_DEV, WORDS)

    def step(total, words):
        plus = unpack(words)
        inner = jnp.dot(signs, plus.T, preferred_element_type=jnp.float32)
        ham = (D - inner) * 0.5
        above = jnp.stack([jnp.sum((ham >= limits[k]).astype(jnp.float32), axis=1) for k in range(NBINS + 1)], axis=1)
        return total + above, None

    above, _ = lax.scan(step, jnp.zeros((QUERIES, NBINS + 1), jnp.float32), blocks)
    counts = above[:, :-1] - above[:, 1:]
    hist = counts * (NBINS / TOTAL_ROWS)
    picked = quant_rows[candidates].astype(jnp.float32)
    raw = jnp.einsum("qd,qjd->qj", queries.astype(jnp.float32), picked, precision=lax.Precision.HIGHEST)
    slots = jnp.arange(CAND, dtype=jnp.int32)
    live = slots[None, :] < shortlist[:, None]
    scores = jnp.where(live, raw * row_scale[candidates], 0.0)
    return hist, scores
```

```python
import functools

import jax
import jax.numpy as jnp
from jax import lax
from jax.experimental import pallas as pl
from jax.experimental.pallas import tpu as pltpu
from jax.sharding import PartitionSpec as P

LANES = 128
F32, BF16, I32, I16 = jnp.float32, jnp.bfloat16, jnp.int32, jnp.int16


def pack_kernel(peers, q_ref, cand_ref, len_ref, out_ref):
    own, width = q_ref.shape
    slots = cand_ref.shape[1]
    vregs = width // LANES
    rows = out_ref.shape[0] // peers
    lens = len_ref[...]
    cand = cand_ref[...]
    slot = lax.broadcasted_iota(I32, cand.shape, 1)
    wide = jnp.where(slot < lens, cand, -1).astype(F32)
    wide = jnp.concatenate([wide, jnp.full((own, LANES - slots), -1.0, F32)], axis=1)
    parts = [q_ref[i : i + 1, v * LANES : (v + 1) * LANES] for i in range(own) for v in range(vregs)]
    parts.append(wide)
    fill = rows - own * vregs - own
    parts.append(jnp.zeros((fill, LANES), F32))
    block = jnp.concatenate(parts, axis=0)
    for p in range(peers):
        out_ref[p * rows : (p + 1) * rows, :] = block


def main_kernel(peers, own, width, slots, nedges, base_ref, edges_ref, x_ref, codes_ref, quant_ref, scale_ref, out_ref, signs_s, qhl_s, bits_s, idx_s, cnt_s, sc_s, inner_s):
    step = pl.program_id(0)
    steps = pl.num_programs(0)
    nq = peers * own
    vregs = width // LANES
    rows = x_ref.shape[0] // peers
    chunk = quant_ref.shape[0]
    words = codes_ref.shape[1]
    reps = LANES // words

    @pl.when(step == 0)
    def _():
        d = lax.broadcasted_iota(I32, (width, 1), 0)
        w, k = d // 32, d % 32
        h, t, c = k // 16, (k % 16) // reps, k % reps
        dest = h * (width // 2) + t * LANES + c * words + w
        plain = []
        for ql in range(own):
            row = jnp.concatenate(
                [x_ref[pl.ds(ql * vregs + v, peers, stride=rows), :] for v in range(vregs)], axis=1
            )
            plain.append(row)
            hi = row.astype(BF16)
            lo = (row - hi.astype(F32)).astype(BF16)
            qhl_s[ql * peers : (ql + 1) * peers, :] = hi
            qhl_s[nq + ql * peers : nq + (ql + 1) * peers, :] = lo
            idx = x_ref[pl.ds(own * vregs + ql, peers, stride=rows), :].astype(I32)
            idx_s[ql * peers : (ql + 1) * peers, :] = jnp.where(idx < 0, -1, idx - base_ref[0])
        full = jnp.concatenate(plain, axis=0)
        signs = jnp.where(full >= 0, 1.0, -1.0).astype(BF16)
        for j in range(width // LANES):
            lane = lax.broadcasted_iota(I32, (1, LANES), 1) + j * LANES
            perm = jnp.where(dest == lane, 1.0, 0.0).astype(BF16)
            signs_s[:, j * LANES : (j + 1) * LANES] = jnp.dot(
                signs, perm, preferred_element_type=F32
            ).astype(BF16)
        cnt_s[...] = jnp.zeros(cnt_s.shape, I16)
        sc_s[...] = jnp.zeros(sc_s.shape, F32)

    lane = lax.broadcasted_iota(I32, (1, LANES), 1)
    sub = lane // words
    word = codes_ref[...]
    tiled = jnp.concatenate([word] * reps, axis=1)
    halves = (tiled.astype(I16), lax.shift_right_logical(tiled, 16).astype(I16))
    for h in range(2):
        for t in range(16 // reps):
            bit = jnp.left_shift(1, t * reps + sub)
            mask = jnp.broadcast_to(bit, (16, LANES)).astype(I16)
            mask = jnp.concatenate([mask] * (chunk // 16), axis=0)
            on = (halves[h] & mask) != 0
            col = h * (width // 2) + t * LANES
            bits_s[:, col : col + LANES] = jnp.where(on, BF16(1), BF16(-1))
    inner = lax.dot_general(
        signs_s[...], bits_s[...], (((1,), (1,)), ((), ())), preferred_element_type=F32
    )
    inner_s[...] = inner.astype(I32).astype(I16)
    for g in range(nq // 16):
        cols = [inner_s[g * 16 : (g + 1) * 16, j * LANES : (j + 1) * LANES] for j in range(chunk // LANES)]
        for k in range(nedges):
            thr = jnp.full((16, LANES), width - 2 * edges_ref[k], I32).astype(I16)
            tot = None
            for x in cols:
                one = jnp.where(x <= thr, I16(1), I16(0))
                tot = one if tot is None else tot + one
            cnt_s[k, g * 16 : (g + 1) * 16, :] += tot
    prod = lax.dot_general(
        qhl_s[...], quant_ref[...], (((1,), (1,)), ((), ())), preferred_element_type=F32
    )
    idx = idx_s[...]
    low = idx & (LANES - 1)
    high = idx >> 7
    acc = sc_s[...]
    for j in range(chunk // LANES):
        s = (prod[:nq, j * LANES : (j + 1) * LANES] + prod[nq:, j * LANES : (j + 1) * LANES]) * scale_ref[:, j * LANES : (j + 1) * LANES]
        got = jnp.take_along_axis(s, low, axis=1, mode="promise_in_bounds")
        acc = jnp.where(high == step * (chunk // LANES) + j, got, acc)
    sc_s[...] = acc

    @pl.when(step == steps - 1)
    def _():
        res = sc_s[...]
        lane = lax.broadcasted_iota(I32, (nq, LANES), 1)
        prev = None
        for k in range(nedges):
            above = jnp.sum(cnt_s[k].astype(I32).astype(F32), axis=1, keepdims=True)
            if k:
                res = jnp.where(lane == LANES // 2 + k - 1, prev - above, res)
            prev = above
        for ql in range(own):
            out_ref[pl.ds(ql, peers, stride=own), :] = res[ql * peers : (ql + 1) * peers, :]


def shards(peers, queries, codes, quant_rows, row_scale, candidates, shortlist, edges):
    own, width = queries.shape
    slots = candidates.shape[1]
    count_rows, words = codes.shape
    nedges = edges.shape[0]
    nbins = nedges - 1
    nq = own * peers
    rows = -(-(own * (width // LANES) + own) // 8) * 8
    chunk = 1024
    payload = pl.pallas_call(
        functools.partial(pack_kernel, peers),
        out_shape=jax.ShapeDtypeStruct((peers * rows, LANES), F32),
        name="pack",
    )(queries, candidates, shortlist.reshape(own, 1))
    got = lax.all_to_all(payload, "corpus", 0, 0, tiled=True)
    base = (lax.axis_index("corpus") * count_rows).astype(I32).reshape(1)
    part = pl.pallas_call(
        functools.partial(main_kernel, peers, own, width, slots, nedges),
        grid=(count_rows // chunk,),
        in_specs=[
            pl.BlockSpec(memory_space=pltpu.SMEM),
            pl.BlockSpec(memory_space=pltpu.SMEM),
            pl.BlockSpec((peers * rows, LANES), lambda i: (0, 0)),
            pl.BlockSpec((chunk, words), lambda i: (i, 0)),
            pl.BlockSpec((chunk, width), lambda i: (i, 0)),
            pl.BlockSpec((1, chunk), lambda i: (0, i)),
        ],
        out_specs=pl.BlockSpec((nq, LANES), lambda i: (0, 0)),
        out_shape=jax.ShapeDtypeStruct((nq, LANES), F32),
        scratch_shapes=[
            pltpu.VMEM((nq, width), BF16),
            pltpu.VMEM((2 * nq, width), BF16),
            pltpu.VMEM((chunk, width), BF16),
            pltpu.VMEM((nq, LANES), I32),
            pltpu.VMEM((nedges, nq, LANES), I16),
            pltpu.VMEM((nq, LANES), F32),
            pltpu.VMEM((nq, chunk), I16),
        ],
        name="main",
    )(base, edges, got, codes, quant_rows, row_scale.reshape(1, count_rows))
    back = lax.all_to_all(part, "corpus", 0, 0, tiled=True)
    total = jnp.sum(back.reshape(peers, own, LANES), axis=0)
    hist = total[:, LANES // 2 : LANES // 2 + nbins] * (nbins / (count_rows * peers))
    return hist, total[:, :slots]


def solution(mesh):
    both = ("corpus", "batch")
    return jax.shard_map(
        functools.partial(shards, mesh.shape["corpus"]),
        mesh=mesh,
        in_specs=(P(both, None), P("corpus", None), P("corpus", None), P("corpus"), P(both, None), P(both), P()),
        out_specs=(P(both, None), P(both, None)),
        check_vma=False,
    )
```

```python
import functools

import jax
import jax.numpy as jnp
from jax import lax
from jax.experimental import pallas as pl
from jax.experimental.pallas import tpu as pltpu
from jax.sharding import PartitionSpec as P

LANES = 128
TILE = 256
F32, BF16, I32, I16, F8 = jnp.float32, jnp.bfloat16, jnp.int32, jnp.int16, jnp.float8_e4m3fn
VMEM = pl.BlockSpec(memory_space=pltpu.VMEM)
SMEM = pl.BlockSpec(memory_space=pltpu.SMEM)
HBM = pl.BlockSpec(memory_space=pltpu.HBM)


def near(x):
    return pltpu.with_memory_space_constraint(x, pltpu.VMEM)


def far(x):
    return pltpu.with_memory_space_constraint(x, pltpu.HBM)


def pack_kernel(peers, q_ref, cand_ref, len_ref, out_ref):
    own, width = q_ref.shape
    slots = cand_ref.shape[1]
    vregs = width // LANES
    rows = out_ref.shape[0] // peers
    slot = lax.broadcasted_iota(I32, (1, slots), 1)
    parts = [q_ref[i : i + 1, v * LANES : (v + 1) * LANES] for i in range(own) for v in range(vregs)]
    for i in range(own):
        live = jnp.where(slot < len_ref[i], cand_ref[i : i + 1, :], -1).astype(F32)
        parts.append(jnp.concatenate([live, jnp.full((1, LANES - slots), -1.0, F32)], axis=1))
    fill = rows - own * vregs - own
    if fill:
        parts.append(jnp.zeros((fill, LANES), F32))
    block = jnp.concatenate(parts, axis=0)
    for p in range(peers):
        out_ref[p * rows : (p + 1) * rows, :] = block


def unpack(word):
    blocks = []
    for h in range(2):
        half = lax.shift_right_logical(word, 16 * h).astype(I16)
        planes = []
        for k in range(16):
            bit = jnp.int16(-(2**15) if k == 15 else 1 << k)
            planes.append(jnp.where((half & bit) != 0, BF16(1), BF16(-1)))
        blocks.append(jnp.concatenate(planes, axis=0).astype(F8))
    return blocks


def main_kernel(peers, own, cols, edges_ref, x_ref, codes_hbm, quant_hbm, scale_hbm, out_ref, codes_ref, quant_ref, scale_ref, signs_s, qhl_s, bits_s, place_s, sems):
    first = [
        pltpu.make_async_copy(codes_hbm, codes_ref, sems.at[0]),
        pltpu.make_async_copy(scale_hbm, scale_ref, sems.at[1]),
    ]
    stream = []
    for i in range(quant_hbm.shape[0] // cols):
        at = pl.ds(i * cols, cols)
        stream.append(pltpu.make_async_copy(quant_hbm.at[at, :], quant_ref.at[at, :], sems.at[2 + i]))
    for copy in first + stream:
        copy.start()
    nq = peers * own
    count, width = quant_ref.shape
    vregs = width // LANES
    rows = x_ref.shape[0] // peers
    nedges = edges_ref.shape[0]
    nbins = nedges - 1
    full, index = [], []
    for i in range(own):
        full.append(
            jnp.concatenate([x_ref[pl.ds(i * vregs + v, peers, stride=rows), :] for v in range(vregs)], axis=1)
        )
        index.append(x_ref[pl.ds(own * vregs + i, peers, stride=rows), :].astype(I32))
    full = jnp.concatenate(full, axis=0)
    index = jnp.concatenate(index, axis=0)
    index = jnp.where(index < 0, -1, index - lax.axis_index("corpus") * count)
    low = index & (LANES - 1)
    high = index >> 7
    hi = full.astype(BF16)
    qhl_s[:nq, :] = hi
    qhl_s[nq:, :] = (full - hi.astype(F32)).astype(BF16)
    signs = jnp.where(full >= 0, -0.5, 0.5).astype(BF16)
    src = lax.broadcasted_iota(I32, (2 * TILE, TILE), 0)
    dst = lax.broadcasted_iota(I32, (2 * TILE, TILE), 1)
    for h in range(2):
        perm = jnp.where(src == (dst & 15) * 32 + 16 * h + (dst >> 4), 1.0, 0.0).astype(BF16)
        for b in range(width // (2 * TILE)):
            at = (2 * b + h) * TILE
            signs_s[:, at : at + TILE] = jnp.dot(
                signs[:, 2 * b * TILE : (2 * b + 2) * TILE], perm, preferred_element_type=F32
            ).astype(F8)
    lane = lax.broadcasted_iota(I32, (LANES, LANES), 1)
    for k in range(nbins):
        place_s[k * LANES : (k + 1) * LANES, :] = jnp.where(lane == LANES // 2 + k, 1.0, 0.0).astype(BF16)

    floor = edges_ref[0] - 1
    dist = lax.broadcasted_iota(I32, (8, LANES), 1) + floor
    tables = []
    for j in range(-(-nbins // 4)):
        word = jnp.zeros((8, LANES), I32)
        for k in range(4 * j, min(4 * j + 4, nbins)):
            inside = (dist >= edges_ref[k]) & (dist < edges_ref[k + 1])
            word = word + jnp.where(inside, jnp.int32(1 << (8 * (k - 4 * j))), 0)
        tables.append(jnp.concatenate([word] * (nq // 8), axis=0))
    offset = (width // 2 - floor).astype(F32)
    tally = [jnp.zeros((nq, LANES), I32) for _ in tables]
    scores = jnp.zeros((nq, LANES), F32)
    for copy in first:
        copy.wait()
    for i in range(count // cols):
        at = slice(i * cols, (i + 1) * cols)
        for b in range(width // (2 * TILE)):
            for h, block in enumerate(unpack(codes_ref[16 * b : 16 * b + 16, at])):
                bits_s[(2 * b + h) * TILE : (2 * b + h + 1) * TILE, at] = block
        half = jnp.dot(signs_s[...], bits_s[:, at], preferred_element_type=F32)
        stream[i].wait()
        prod = lax.dot_general(
            qhl_s[...], quant_ref[at, :], (((1,), (1,)), ((), ())), preferred_element_type=F32
        )
        for j in range(cols // LANES):
            cut = slice(j * LANES, (j + 1) * LANES)
            where = jnp.clip(half[:, cut] + offset, 0.0, LANES - 1.0).astype(I32)
            tally = [
                t + jnp.take_along_axis(w, where, axis=1, mode="promise_in_bounds") for t, w in zip(tally, tables)
            ]
            row = i * (cols // LANES) + j
            value = (prod[:nq, cut] + prod[nq:, cut]) * scale_ref[:, row * LANES : (row + 1) * LANES]
            value = jnp.take_along_axis(value, low, axis=1, mode="promise_in_bounds")
            scores = jnp.where(high == row, value, scores)
    planes = []
    for k in range(nbins):
        planes.append(((tally[k // 4] >> (8 * (k % 4))) & 255).astype(F32).astype(BF16))
    counts = jnp.dot(jnp.concatenate(planes, axis=1), place_s[...], preferred_element_type=F32)
    lane = lax.broadcasted_iota(I32, (nq, LANES), 1)
    res = jnp.where(lane < LANES // 2, scores, counts)
    for i in range(own):
        out_ref[pl.ds(i, peers, stride=own), :] = res[i * peers : (i + 1) * peers, :]


def shards(peers, queries, codes, quant_rows, row_scale, candidates, shortlist, edges):
    own, width = queries.shape
    slots = candidates.shape[1]
    count, words = codes.shape
    nbins = edges.shape[0] - 1
    nq = own * peers
    rows = -(-(own * (width // LANES) + own) // 8) * 8
    assert words % 16 == 0 and width == 32 * words and count % 512 == 0
    assert count // LANES < 256 and slots <= LANES // 2 and nbins <= LANES // 2
    payload = pl.pallas_call(
        functools.partial(pack_kernel, peers),
        in_specs=[VMEM, VMEM, SMEM],
        out_specs=VMEM,
        out_shape=pltpu.VMEM((peers * rows, LANES), F32),
        name="pack",
    )(far(queries), far(candidates), far(shortlist))
    got = lax.all_to_all(payload, "corpus", 0, 0, tiled=True)
    part = pl.pallas_call(
        functools.partial(main_kernel, peers, own, 512),
        in_specs=[SMEM, VMEM, HBM, HBM, HBM],
        out_specs=VMEM,
        out_shape=pltpu.VMEM((nq, LANES), F32),
        scratch_shapes=[
            pltpu.VMEM((words, count), I32),
            pltpu.VMEM((count, width), BF16),
            pltpu.VMEM((1, count), F32),
            pltpu.VMEM((nq, width), F8),
            pltpu.VMEM((2 * nq, width), BF16),
            pltpu.VMEM((width, count), F8),
            pltpu.VMEM((nbins * LANES, LANES), BF16),
            pltpu.SemaphoreType.DMA((2 + count // 512,)),
        ],
        compiler_params=pltpu.CompilerParams(vmem_limit_bytes=48 << 20),
        cost_estimate=pl.CostEstimate(flops=4 * 10**9, bytes_accessed=0, transcendentals=0),
        name="main",
    )(far(edges), near(got), far(codes.T), far(quant_rows), far(row_scale.reshape(1, count)))
    back = lax.all_to_all(part, "corpus", 0, 0, tiled=True)
    total = jnp.sum(back.reshape(peers, own, LANES), axis=0)
    hist = total[:, LANES // 2 : LANES // 2 + nbins] * (nbins / (count * peers))
    return hist, total[:, :slots]


def solution(mesh):
    both = ("corpus", "batch")
    return jax.shard_map(
        functools.partial(shards, mesh.shape["corpus"]),
        mesh=mesh,
        in_specs=(P(both, None), P("corpus", None), P("corpus", None), P("corpus"), P(both, None), P(both), P()),
        out_specs=(P(both, None), P(both, None)),
        check_vma=False,
    )
```

```python
import functools
import math

import jax
import jax.numpy as jnp
from jax import lax
from jax.experimental import pallas as pl
from jax.experimental.pallas import tpu as pltpu
from jax.sharding import PartitionSpec as P

LANES = 128
TILE = 256
F32, BF16, I32, I16, F8 = jnp.float32, jnp.bfloat16, jnp.int32, jnp.int16, jnp.float8_e4m3fn
VMEM = pl.BlockSpec(memory_space=pltpu.VMEM)
SMEM = pl.BlockSpec(memory_space=pltpu.SMEM)
ANY = pl.BlockSpec(memory_space=pl.ANY)


def near(x):
    return pltpu.with_memory_space_constraint(x, pltpu.VMEM)


def far(x):
    return pltpu.with_memory_space_constraint(x, pltpu.HBM)


def pack_kernel(peers, q_hbm, cand_hbm, len_hbm, edges_hbm, out_ref, table_ref, q_ref, cand_ref, len_ref, edges_ref, sems):
    pairs = [(q_hbm, q_ref), (cand_hbm, cand_ref), (len_hbm, len_ref), (edges_hbm, edges_ref)]
    moves = [pltpu.make_async_copy(*pair, sems.at[n]) for n, pair in enumerate(pairs)]
    for move in moves:
        move.start()
    for move in moves:
        move.wait()
    own, width = q_ref.shape
    slots = cand_ref.shape[1]
    rows = out_ref.shape[0] // peers
    slot = lax.broadcasted_iota(I32, (1, slots), 1)
    dead = jnp.full((1, LANES // 2 - slots), -1.0, F32)
    parts = [q_ref[i : i + 1, v * LANES : (v + 1) * LANES] for i in range(own) for v in range(width // LANES)]
    lists = []
    for i in range(own):
        lists += [jnp.where(slot < len_ref[i], cand_ref[i : i + 1, :], -1).astype(F32), dead]
    for i in range(0, own, 2):
        parts.append(jnp.concatenate(lists[2 * i : 2 * i + 4], axis=1))
    block = jnp.concatenate(parts, axis=0)
    for p in range(peers):
        out_ref[p * rows : (p + 1) * rows, :] = block
    nbins = edges_ref.shape[0] - 1
    floor = edges_ref[0] - 1
    dist = lax.broadcasted_iota(I32, (8, LANES), 1) + floor
    for j in range(-(-nbins // 4)):
        word = jnp.zeros((8, LANES), I32)
        for k in range(4 * j, min(4 * j + 4, nbins)):
            inside = (dist >= edges_ref[k]) & (dist < edges_ref[k + 1])
            word = word + jnp.where(inside, jnp.int32(1 << (8 * (k - 4 * j))), 0)
        table_ref[8 * j : 8 * j + 8, :] = word
    table_ref[-8:, :] = jnp.full((8, LANES), width // 2 - floor, I32)


def unpack(word):
    blocks = []
    for h in range(2):
        half = lax.shift_right_logical(word, 16 * h).astype(I16)
        planes = []
        for k in range(16):
            bit = jnp.int16(-(2**15) if k == 15 else 1 << k)
            planes.append(jnp.where((half & bit) != 0, BF16(1), BF16(-1)))
        blocks.append(jnp.concatenate(planes, axis=0).astype(F8))
    return blocks


def main_kernel(own, group, cols, nbins, table_ref, x_ref, codes_ref, quant_ref, scale_ref, out_ref, signs_s, qhl_s, bits_s, place_s):
    count, width = quant_ref.shape
    vregs = width // LANES
    rows = own * vregs + -(-own // 2)
    peers = x_ref.shape[0] // rows
    nq = group * own
    src = lax.broadcasted_iota(I32, (2 * TILE, TILE), 0)
    dst = lax.broadcasted_iota(I32, (2 * TILE, TILE), 1)
    perms = [jnp.where(src == (dst & 15) * 32 + 16 * h + (dst >> 4), 1.0, 0.0).astype(BF16) for h in range(2)]
    lane = lax.broadcasted_iota(I32, (LANES, LANES), 1)
    for k in range(nbins):
        place_s[k * LANES : (k + 1) * LANES, :] = jnp.where(lane == LANES // 2 + k, 1.0, 0.0).astype(BF16)
    tables = [
        jnp.concatenate([table_ref[8 * j : 8 * j + 8, :]] * (nq // 8), axis=0) for j in range(table_ref.shape[0] // 8 - 1)
    ]
    offset = jnp.concatenate([table_ref[-8:, :].astype(F32)] * (nq // 8), axis=0)

    def serve(start):
        lane = lax.broadcasted_iota(I32, (group, LANES), 1)
        full, index = [], []
        for i in range(own):
            at = start * rows + i * vregs
            full.append(jnp.concatenate([x_ref[pl.ds(at + v, group, stride=rows), :] for v in range(vregs)], axis=1))
            got = x_ref[pl.ds(start * rows + own * vregs + i // 2, group, stride=rows), :]
            if i % 2:
                got = pltpu.roll(got, LANES // 2, 1)
            index.append(jnp.where(lane < LANES // 2, got, -1.0).astype(I32))
        full = jnp.concatenate(full, axis=0)
        index = jnp.concatenate(index, axis=0)
        index = jnp.where(index < 0, -1, index - lax.axis_index("corpus") * count)
        low = index & (LANES - 1)
        high = index >> 7
        hi = full.astype(BF16)
        qhl_s[:nq, :] = hi
        qhl_s[nq:, :] = (full - hi.astype(F32)).astype(BF16)
        signs = jnp.where(full >= 0, -0.5, 0.5).astype(BF16)
        for h in range(2):
            for b in range(width // (2 * TILE)):
                at = (2 * b + h) * TILE
                signs_s[:, at : at + TILE] = jnp.dot(
                    signs[:, 2 * b * TILE : (2 * b + 2) * TILE], perms[h], preferred_element_type=F32
                ).astype(F8)

        tally = [jnp.zeros((nq, LANES), I32) for _ in tables]
        scores = jnp.zeros((nq, LANES), F32)
        for i in range(count // cols):
            at = slice(i * cols, (i + 1) * cols)
            for b in range(width // (2 * TILE)):
                for h, block in enumerate(unpack(codes_ref[16 * b : 16 * b + 16, at])):
                    bits_s[(2 * b + h) * TILE : (2 * b + h + 1) * TILE, at] = block
            half = jnp.dot(signs_s[...], bits_s[:, at], preferred_element_type=F32)
            prod = lax.dot_general(
                qhl_s[...], quant_ref[at, :], (((1,), (1,)), ((), ())), preferred_element_type=F32
            )
            for j in range(cols // LANES):
                cut = slice(j * LANES, (j + 1) * LANES)
                where = jnp.clip(half[:, cut] + offset, 0.0, LANES - 1.0).astype(I32)
                tally = [
                    t + jnp.take_along_axis(w, where, axis=1, mode="promise_in_bounds") for t, w in zip(tally, tables)
                ]
                row = i * (cols // LANES) + j
                value = (prod[:nq, cut] + prod[nq:, cut]) * scale_ref[:, row * LANES : (row + 1) * LANES]
                value = jnp.take_along_axis(value, low, axis=1, mode="promise_in_bounds")
                scores = jnp.where(high == row, value, scores)
        planes = [((tally[k // 4] >> (8 * (k % 4))) & 255).astype(F32).astype(BF16) for k in range(nbins)]
        counts = jnp.dot(jnp.concatenate(planes, axis=1), place_s[...], preferred_element_type=F32)
        lane = lax.broadcasted_iota(I32, (nq, LANES), 1)
        res = jnp.where(lane < LANES // 2, scores, counts)
        for i in range(own):
            out_ref[pl.ds(start * own + i, group, stride=own), :] = res[i * group : (i + 1) * group, :]

    if peers == group:
        serve(0)
    else:
        pl.loop(0, peers // group)(lambda g: serve(g * group))


def shards(peers, queries, codes, quant_rows, row_scale, candidates, shortlist, edges):
    own, width = queries.shape
    slots = candidates.shape[1]
    count, words = codes.shape
    nbins = edges.shape[0] - 1
    nq = own * peers
    cols = 768 if count % 768 == 0 else 512
    group = math.gcd(peers, 16)
    part = group * own
    rows = own * (width // LANES) + -(-own // 2)
    assert words % 16 == 0 and width == 32 * words and count % 512 == 0
    assert count // LANES < 256 and slots <= LANES // 2 and nbins <= LANES // 2
    payload, table = pl.pallas_call(
        functools.partial(pack_kernel, peers),
        in_specs=[ANY, ANY, ANY, ANY],
        out_specs=[VMEM, VMEM],
        out_shape=[
            pltpu.VMEM((peers * rows, LANES), F32),
            pltpu.VMEM((8 * -(-nbins // 4) + 8, LANES), I32),
        ],
        scratch_shapes=[
            pltpu.VMEM(queries.shape, F32),
            pltpu.VMEM(candidates.shape, I32),
            pltpu.SMEM(shortlist.shape, I32),
            pltpu.SMEM(edges.shape, I32),
            pltpu.SemaphoreType.DMA((4,)),
        ],
        compiler_params=pltpu.CompilerParams(vmem_limit_bytes=2 << 20),
        cost_estimate=pl.CostEstimate(flops=10**10, bytes_accessed=0, transcendentals=0),
        name="pack",
    )(far(queries), far(candidates), far(shortlist), far(edges))
    got = lax.all_to_all(payload.reshape(peers, 1, rows * LANES), "corpus", 0, 0)
    got = got.reshape(peers * rows, LANES)
    result = pl.pallas_call(
        functools.partial(main_kernel, own, group, cols, nbins),
        in_specs=[VMEM, VMEM, VMEM, VMEM, VMEM],
        out_specs=VMEM,
        out_shape=pltpu.VMEM((nq, LANES), F32),
        scratch_shapes=[
            pltpu.VMEM((part, width), F8),
            pltpu.VMEM((2 * part, width), BF16),
            pltpu.VMEM((width, count), F8),
            pltpu.VMEM((nbins * LANES, LANES), BF16),
        ],
        compiler_params=pltpu.CompilerParams(vmem_limit_bytes=24 << 20),
        cost_estimate=pl.CostEstimate(flops=4 * 10**9, bytes_accessed=0, transcendentals=0),
        name="main",
    )(near(table), near(got), codes.T, quant_rows, row_scale.reshape(1, count))
    back = lax.all_to_all(result, "corpus", 0, 0, tiled=True)
    total = jnp.sum(back.reshape(peers, own, LANES), axis=0)
    hist = total[:, LANES // 2 : LANES // 2 + nbins] * (nbins / (count * peers))
    return hist, total[:, :slots]


def solution(mesh):
    both = ("corpus", "batch")
    return jax.shard_map(
        functools.partial(shards, mesh.shape["corpus"]),
        mesh=mesh,
        in_specs=(P(both, None), P("corpus", None), P("corpus", None), P("corpus"), P(both, None), P(both), P()),
        out_specs=(P(both, None), P(both, None)),
        check_vma=False,
    )
```

```python
import functools
import math

import jax
import jax.numpy as jnp
from jax import lax
from jax.experimental import pallas as pl
from jax.experimental.pallas import tpu as pltpu
from jax.sharding import PartitionSpec as P

LANES = 128
TILE = 256
F32, BF16, I32, I16, F8 = jnp.float32, jnp.bfloat16, jnp.int32, jnp.int16, jnp.float8_e4m3fn
VMEM = pl.BlockSpec(memory_space=pltpu.VMEM)
SMEM = pl.BlockSpec(memory_space=pltpu.SMEM)
ANY = pl.BlockSpec(memory_space=pl.ANY)


def near(x):
    return pltpu.with_memory_space_constraint(x, pltpu.VMEM)


def far(x):
    return pltpu.with_memory_space_constraint(x, pltpu.HBM)


def pack_kernel(share, q_hbm, cand_hbm, len_hbm, edges_hbm, out_ref, table_ref, q_ref, cand_ref, len_ref, edges_ref, sems):
    pairs = [(q_hbm, q_ref), (cand_hbm, cand_ref), (len_hbm, len_ref), (edges_hbm, edges_ref)]
    moves = [pltpu.make_async_copy(*pair, sems.at[n]) for n, pair in enumerate(pairs)]
    for move in moves:
        move.start()
    for move in moves:
        move.wait()
    own, width = q_ref.shape
    slots = cand_ref.shape[1]
    slot = lax.broadcasted_iota(I32, (1, slots), 1)
    dead = jnp.full((1, LANES // 2 - slots), -1.0, F32)
    parts = []
    for first in range(0, own, share):
        lists = []
        for i in range(first, first + share):
            parts += [q_ref[i : i + 1, v * LANES : (v + 1) * LANES] for v in range(width // LANES)]
            lists += [jnp.where(slot < len_ref[i], cand_ref[i : i + 1, :], -1).astype(F32), dead]
        for i in range(0, share, 2):
            parts.append(jnp.concatenate(lists[2 * i : 2 * i + 4], axis=1))
    block = jnp.concatenate(parts, axis=0)
    rows = block.shape[0]
    for p in range(out_ref.shape[0] // rows):
        out_ref[p * rows : (p + 1) * rows, :] = block
    nbins = edges_ref.shape[0] - 1
    floor = edges_ref[0] - 1
    dist = lax.broadcasted_iota(I32, (8, LANES), 1) + floor
    for j in range(-(-nbins // 4)):
        word = jnp.zeros((8, LANES), I32)
        for k in range(4 * j, min(4 * j + 4, nbins)):
            inside = (dist >= edges_ref[k]) & (dist < edges_ref[k + 1])
            word = word + jnp.where(inside, jnp.int32(1 << (8 * (k - 4 * j))), 0)
        table_ref[8 * j : 8 * j + 8, :] = word
    table_ref[-8:, :] = jnp.full((8, LANES), width // 2 - floor, I32)


def unpack(word):
    blocks = []
    for h in range(2):
        half = lax.shift_right_logical(word, 16 * h).astype(I16)
        planes = []
        for k in range(16):
            bit = jnp.int16(-(2**15) if k == 15 else 1 << k)
            planes.append(jnp.where((half & bit) != 0, BF16(1), BF16(-1)))
        blocks.append(jnp.concatenate(planes, axis=0).astype(F8))
    return blocks


def main_kernel(share, group, cols, nbins, table_ref, x_ref, codes_ref, quant_ref, scale_ref, out_ref, signs_s, qhl_s, bits_s, place_s):
    count, width = quant_ref.shape
    vregs = width // LANES
    rows = share * vregs + share // 2
    sources = x_ref.shape[0] // rows
    nq = group * share
    src = lax.broadcasted_iota(I32, (2 * TILE, TILE), 0)
    dst = lax.broadcasted_iota(I32, (2 * TILE, TILE), 1)
    perms = [jnp.where(src == (dst & 15) * 32 + 16 * h + (dst >> 4), 1.0, 0.0).astype(BF16) for h in range(2)]
    lane = lax.broadcasted_iota(I32, (LANES, LANES), 1)
    for k in range(nbins):
        place_s[k * LANES : (k + 1) * LANES, :] = jnp.where(lane == LANES // 2 + k, 1.0, 0.0).astype(BF16)
    tables = [
        jnp.concatenate([table_ref[8 * j : 8 * j + 8, :]] * (nq // 8), axis=0) for j in range(table_ref.shape[0] // 8 - 1)
    ]
    offset = jnp.concatenate([table_ref[-8:, :].astype(F32)] * (nq // 8), axis=0)

    def serve(start):
        lane = lax.broadcasted_iota(I32, (group, LANES), 1)
        full, index = [], []
        for i in range(share):
            at = start * rows + i * vregs
            full.append(jnp.concatenate([x_ref[pl.ds(at + v, group, stride=rows), :] for v in range(vregs)], axis=1))
            got = x_ref[pl.ds(start * rows + share * vregs + i // 2, group, stride=rows), :]
            if i % 2:
                got = pltpu.roll(got, LANES // 2, 1)
            index.append(jnp.where(lane < LANES // 2, got, -1.0).astype(I32))
        full = jnp.concatenate(full, axis=0)
        index = jnp.concatenate(index, axis=0)
        index = jnp.where(index < 0, -1, index - lax.axis_index("corpus") * count)
        low = index & (LANES - 1)
        high = index >> 7
        hi = full.astype(BF16)
        qhl_s[:nq, :] = hi
        qhl_s[nq:, :] = (full - hi.astype(F32)).astype(BF16)
        signs = jnp.where(full >= 0, -0.5, 0.5).astype(BF16)
        for h in range(2):
            for b in range(width // (2 * TILE)):
                at = (2 * b + h) * TILE
                signs_s[:, at : at + TILE] = jnp.dot(
                    signs[:, 2 * b * TILE : (2 * b + 2) * TILE], perms[h], preferred_element_type=F32
                ).astype(F8)

        tally = [jnp.zeros((nq, LANES), I32) for _ in tables]
        scores = jnp.zeros((nq, LANES), F32)
        for i in range(count // cols):
            at = slice(i * cols, (i + 1) * cols)
            for b in range(width // (2 * TILE)):
                for h, block in enumerate(unpack(codes_ref[16 * b : 16 * b + 16, at])):
                    bits_s[(2 * b + h) * TILE : (2 * b + h + 1) * TILE, at] = block
            half = jnp.dot(signs_s[...], bits_s[:, at], preferred_element_type=F32)
            prod = lax.dot_general(
                qhl_s[...], quant_ref[at, :], (((1,), (1,)), ((), ())), preferred_element_type=F32
            )
            for j in range(cols // LANES):
                cut = slice(j * LANES, (j + 1) * LANES)
                where = jnp.clip(half[:, cut] + offset, 0.0, LANES - 1.0).astype(I32)
                tally = [
                    t + jnp.take_along_axis(w, where, axis=1, mode="promise_in_bounds") for t, w in zip(tally, tables)
                ]
                row = i * (cols // LANES) + j
                value = (prod[:nq, cut] + prod[nq:, cut]) * scale_ref[:, row * LANES : (row + 1) * LANES]
                value = jnp.take_along_axis(value, low, axis=1, mode="promise_in_bounds")
                scores = jnp.where(high == row, value, scores)
        planes = [((tally[k // 4] >> (8 * (k % 4))) & 255).astype(F32).astype(BF16) for k in range(nbins)]
        counts = jnp.dot(jnp.concatenate(planes, axis=1), place_s[...], preferred_element_type=F32)
        lane = lax.broadcasted_iota(I32, (nq, LANES), 1)
        res = jnp.where(lane < LANES // 2, scores, counts)
        for i in range(share):
            out_ref[pl.ds(start * share + i, group, stride=share), :] = res[i * group : (i + 1) * group, :]

    if sources == group:
        serve(0)
    else:
        pl.loop(0, sources // group)(lambda g: serve(g * group))


def shards(chips, cores, queries, codes, quant_rows, row_scale, candidates, shortlist, edges):
    both = ("corpus", "batch")
    own, width = queries.shape
    slots = candidates.shape[1]
    count, words = codes.shape
    nbins = edges.shape[0] - 1
    devices = chips * cores
    share = own // cores
    nq = share * devices
    cols = 768 if count % 768 == 0 else 512
    group = math.gcd(devices, 32)
    part = group * share
    rows = share * (width // LANES) + share // 2
    assert own % (2 * cores) == 0
    assert words % 16 == 0 and width == 32 * words and count % 512 == 0
    assert count // LANES < 256 and slots <= LANES // 2 and nbins <= LANES // 2
    payload, table = pl.pallas_call(
        functools.partial(pack_kernel, share),
        in_specs=[ANY, ANY, ANY, ANY],
        out_specs=[VMEM, VMEM],
        out_shape=[
            pltpu.VMEM((devices * rows, LANES), F32),
            pltpu.VMEM((8 * -(-nbins // 4) + 8, LANES), I32),
        ],
        scratch_shapes=[
            pltpu.VMEM(queries.shape, F32),
            pltpu.VMEM(candidates.shape, I32),
            pltpu.SMEM(shortlist.shape, I32),
            pltpu.SMEM(edges.shape, I32),
            pltpu.SemaphoreType.DMA((4,)),
        ],
        compiler_params=pltpu.CompilerParams(vmem_limit_bytes=2 << 20),
        cost_estimate=pl.CostEstimate(flops=10**10, bytes_accessed=0, transcendentals=0),
        name="pack",
    )(far(queries), far(candidates), far(shortlist), far(edges))
    got = lax.all_to_all(payload.reshape(devices, 1, rows * LANES), both, 0, 0).reshape(devices * rows, LANES)
    result = pl.pallas_call(
        functools.partial(main_kernel, share, group, cols, nbins),
        in_specs=[VMEM, VMEM, VMEM, VMEM, VMEM],
        out_specs=VMEM,
        out_shape=pltpu.VMEM((nq, LANES), F32),
        scratch_shapes=[
            pltpu.VMEM((part, width), F8),
            pltpu.VMEM((2 * part, width), BF16),
            pltpu.VMEM((width, count), F8),
            pltpu.VMEM((nbins * LANES, LANES), BF16),
        ],
        compiler_params=pltpu.CompilerParams(vmem_limit_bytes=24 << 20),
        cost_estimate=pl.CostEstimate(flops=4 * 10**9, bytes_accessed=0, transcendentals=0),
        name="main",
    )(near(table), near(got), codes.T, quant_rows, row_scale.reshape(1, count))
    back = lax.all_to_all(result.reshape(devices, 1, share * LANES), both, 0, 0)
    total = jnp.sum(back.reshape(chips, own, LANES), axis=0)
    hist = total[:, LANES // 2 : LANES // 2 + nbins] * (nbins / (count * chips))
    return hist, total[:, :slots]


def solution(mesh):
    both = ("corpus", "batch")
    return jax.shard_map(
        functools.partial(shards, mesh.shape["corpus"], mesh.shape["batch"]),
        mesh=mesh,
        in_specs=(P(both, None), P("corpus", None), P("corpus", None), P("corpus"), P(both, None), P(both), P()),
        out_specs=(P(both, None), P(both, None)),
        check_vma=False,
    )
```

```python
import functools
import math

import jax
import jax.numpy as jnp
from jax import lax
from jax.experimental import pallas as pl
from jax.experimental.pallas import tpu as pltpu
from jax.sharding import PartitionSpec as P

LANES = 128
TILE = 256
F32, BF16, I32, I16, F8 = jnp.float32, jnp.bfloat16, jnp.int32, jnp.int16, jnp.float8_e4m3fn
VMEM = pl.BlockSpec(memory_space=pltpu.VMEM)
SMEM = pl.BlockSpec(memory_space=pltpu.SMEM)
ANY = pl.BlockSpec(memory_space=pl.ANY)


def near(x):
    return pltpu.with_memory_space_constraint(x, pltpu.VMEM)


def far(x):
    return pltpu.with_memory_space_constraint(x, pltpu.HBM)


def pack_kernel(share, q_ref, cand_ref, len_ref, out_ref):
    own, width = q_ref.shape
    slots = cand_ref.shape[1]
    slot = lax.broadcasted_iota(I32, (1, slots), 1)
    dead = jnp.full((1, LANES // 2 - slots), -1.0, F32)
    parts = []
    for first in range(0, own, share):
        lists = []
        for i in range(first, first + share):
            parts += [q_ref[i : i + 1, v * LANES : (v + 1) * LANES] for v in range(width // LANES)]
            lists += [jnp.where(slot < len_ref[i], cand_ref[i : i + 1, :], -1).astype(F32), dead]
        for i in range(0, share, 2):
            parts.append(jnp.concatenate(lists[2 * i : 2 * i + 4], axis=1))
    block = jnp.concatenate(parts, axis=0)
    rows = block.shape[0]
    for p in range(out_ref.shape[0] // rows):
        out_ref[p * rows : (p + 1) * rows, :] = block


def unpack(word):
    blocks = []
    for h in range(2):
        half = lax.shift_right_logical(word, 16 * h).astype(I16)
        planes = []
        for k in range(16):
            bit = jnp.int16(-(2**15) if k == 15 else 1 << k)
            planes.append(jnp.where((half & bit) != 0, BF16(1), BF16(-1)))
        blocks.append(jnp.concatenate(planes, axis=0).astype(F8))
    return blocks


def main_kernel(share, group, cols, edges_ref, x_ref, codes_ref, quant_ref, scale_ref, out_ref, signs_s, qhl_s, bits_s, place_s):
    count, width = quant_ref.shape
    vregs = width // LANES
    rows = share * vregs + share // 2
    sources = x_ref.shape[0] // rows
    nq = group * share
    nbins = edges_ref.shape[1] - 1
    src = lax.broadcasted_iota(I32, (2 * TILE, TILE), 0)
    dst = lax.broadcasted_iota(I32, (2 * TILE, TILE), 1)
    perms = [jnp.where(src == (dst & 15) * 32 + 16 * h + (dst >> 4), 1.0, 0.0).astype(BF16) for h in range(2)]
    lane = lax.broadcasted_iota(I32, (LANES, LANES), 1)
    for k in range(nbins):
        place_s[k * LANES : (k + 1) * LANES, :] = jnp.where(lane == LANES // 2 + k, 1.0, 0.0).astype(BF16)
    edge = [jnp.broadcast_to(edges_ref[:, k : k + 1], (8, LANES)) for k in range(nbins + 1)]
    dist = lax.broadcasted_iota(I32, (8, LANES), 1) + edge[0] - 1
    tables = []
    for j in range(-(-nbins // 4)):
        word = jnp.zeros((8, LANES), I32)
        for k in range(4 * j, min(4 * j + 4, nbins)):
            inside = (dist >= edge[k]) & (dist < edge[k + 1])
            word = word + jnp.where(inside, jnp.int32(1 << (8 * (k - 4 * j))), 0)
        tables.append(jnp.concatenate([word] * (nq // 8), axis=0))
    offset = jnp.concatenate([(width // 2 + 1 - edge[0]).astype(F32)] * (nq // 8), axis=0)

    def serve(start):
        lane = lax.broadcasted_iota(I32, (group, LANES), 1)
        full, index = [], []
        for i in range(share):
            at = start * rows + i * vregs
            full.append(jnp.concatenate([x_ref[pl.ds(at + v, group, stride=rows), :] for v in range(vregs)], axis=1))
            got = x_ref[pl.ds(start * rows + share * vregs + i // 2, group, stride=rows), :]
            if i % 2:
                got = pltpu.roll(got, LANES // 2, 1)
            index.append(jnp.where(lane < LANES // 2, got, -1.0).astype(I32))
        full = jnp.concatenate(full, axis=0)
        index = jnp.concatenate(index, axis=0)
        index = jnp.where(index < 0, -1, index - lax.axis_index("corpus") * count)
        low = index & (LANES - 1)
        high = index >> 7
        hi = full.astype(BF16)
        qhl_s[:nq, :] = hi
        qhl_s[nq:, :] = (full - hi.astype(F32)).astype(BF16)
        signs = jnp.where(full >= 0, -0.5, 0.5).astype(BF16)
        for h in range(2):
            for b in range(width // (2 * TILE)):
                at = (2 * b + h) * TILE
                signs_s[:, at : at + TILE] = jnp.dot(
                    signs[:, 2 * b * TILE : (2 * b + 2) * TILE], perms[h], preferred_element_type=F32
                ).astype(F8)

        tally = [jnp.zeros((nq, LANES), I32) for _ in tables]
        scores = jnp.zeros((nq, LANES), F32)
        for i in range(count // cols):
            at = slice(i * cols, (i + 1) * cols)
            for b in range(width // (2 * TILE)):
                for h, block in enumerate(unpack(codes_ref[16 * b : 16 * b + 16, at])):
                    bits_s[(2 * b + h) * TILE : (2 * b + h + 1) * TILE, at] = block
            half = jnp.dot(signs_s[...], bits_s[:, at], preferred_element_type=F32)
            prod = lax.dot_general(
                qhl_s[...], quant_ref[at, :], (((1,), (1,)), ((), ())), preferred_element_type=F32
            )
            for j in range(cols // LANES):
                cut = slice(j * LANES, (j + 1) * LANES)
                where = jnp.clip(half[:, cut] + offset, 0.0, LANES - 1.0).astype(I32)
                tally = [
                    t + jnp.take_along_axis(w, where, axis=1, mode="promise_in_bounds") for t, w in zip(tally, tables)
                ]
                row = i * (cols // LANES) + j
                value = (prod[:nq, cut] + prod[nq:, cut]) * scale_ref[:, row * LANES : (row + 1) * LANES]
                value = jnp.take_along_axis(value, low, axis=1, mode="promise_in_bounds")
                scores = jnp.where(high == row, value, scores)
        planes = [((tally[k // 4] >> (8 * (k % 4))) & 255).astype(F32).astype(BF16) for k in range(nbins)]
        counts = jnp.dot(jnp.concatenate(planes, axis=1), place_s[...], preferred_element_type=F32)
        lane = lax.broadcasted_iota(I32, (nq, LANES), 1)
        res = jnp.where(lane < LANES // 2, scores, counts)
        for i in range(share):
            out_ref[pl.ds(start * share + i, group, stride=share), :] = res[i * group : (i + 1) * group, :]

    if sources == group:
        serve(0)
    else:
        pl.loop(0, sources // group)(lambda g: serve(g * group))


def shards(chips, cores, queries, codes, quant_rows, row_scale, candidates, shortlist, edges):
    both = ("corpus", "batch")
    own, width = queries.shape
    slots = candidates.shape[1]
    count, words = codes.shape
    nbins = edges.shape[0] - 1
    devices = chips * cores
    share = own // cores
    nq = share * devices
    cols = 768 if count % 768 == 0 else 512
    group = math.gcd(devices, 32)
    part = group * share
    rows = share * (width // LANES) + share // 2
    assert own % (2 * cores) == 0
    assert words % 16 == 0 and width == 32 * words and count % 512 == 0
    assert count // LANES < 256 and slots <= LANES // 2 and nbins <= LANES // 2
    payload = pl.pallas_call(
        functools.partial(pack_kernel, share),
        in_specs=[VMEM, VMEM, SMEM],
        out_specs=VMEM,
        out_shape=pltpu.VMEM((devices * rows, LANES), F32),
        compiler_params=pltpu.CompilerParams(vmem_limit_bytes=2 << 20),
        cost_estimate=pl.CostEstimate(flops=10**10, bytes_accessed=0, transcendentals=0),
        name="pack",
    )(far(queries), far(candidates), far(shortlist))
    got = lax.all_to_all(payload.reshape(devices, 1, rows * LANES), both, 0, 0).reshape(devices * rows, LANES)
    result = pl.pallas_call(
        functools.partial(main_kernel, share, group, cols),
        in_specs=[VMEM, VMEM, VMEM, VMEM, VMEM],
        out_specs=VMEM,
        out_shape=pltpu.VMEM((nq, LANES), F32),
        scratch_shapes=[
            pltpu.VMEM((part, width), F8),
            pltpu.VMEM((2 * part, width), BF16),
            pltpu.VMEM((width, count), F8),
            pltpu.VMEM((nbins * LANES, LANES), BF16),
        ],
        compiler_params=pltpu.CompilerParams(vmem_limit_bytes=24 << 20),
        cost_estimate=pl.CostEstimate(flops=4 * 10**9, bytes_accessed=0, transcendentals=0),
        name="main",
    )(near(edges.reshape(1, nbins + 1)), near(got), codes.T, quant_rows, row_scale.reshape(1, count))
    back = lax.all_to_all(result.reshape(devices, 1, share * LANES), both, 0, 0)
    total = jnp.sum(back.reshape(chips, own, LANES), axis=0)
    hist = total[:, LANES // 2 : LANES // 2 + nbins] * (nbins / (count * chips))
    return hist, total[:, :slots]


def solution(mesh):
    both = ("corpus", "batch")
    return jax.shard_map(
        functools.partial(shards, mesh.shape["corpus"], mesh.shape["batch"]),
        mesh=mesh,
        in_specs=(P(both, None), P("corpus", None), P("corpus", None), P("corpus"), P(both, None), P(both), P()),
        out_specs=(P(both, None), P(both, None)),
        check_vma=False,
    )
```

```python
import functools
import math

import jax
import jax.numpy as jnp
from jax import lax
from jax.experimental import pallas as pl
from jax.experimental.pallas import tpu as pltpu
from jax.sharding import PartitionSpec as P

LANES = 128
TILE = 256
F32, BF16, I32, I16, F8 = jnp.float32, jnp.bfloat16, jnp.int32, jnp.int16, jnp.float8_e4m3fn
VMEM = pl.BlockSpec(memory_space=pltpu.VMEM)
SMEM = pl.BlockSpec(memory_space=pltpu.SMEM)
ANY = pl.BlockSpec(memory_space=pl.ANY)


def near(x):
    return pltpu.with_memory_space_constraint(x, pltpu.VMEM)


def far(x):
    return pltpu.with_memory_space_constraint(x, pltpu.HBM)


def pack_kernel(share, q_ref, cand_ref, len_ref, out_ref):
    own, width = q_ref.shape
    slots = cand_ref.shape[1]
    slot = lax.broadcasted_iota(I32, (1, slots), 1)
    dead = jnp.full((1, LANES // 2 - slots), -1.0, F32)
    parts = []
    for first in range(0, own, share):
        lists = []
        for i in range(first, first + share):
            parts += [q_ref[i : i + 1, v * LANES : (v + 1) * LANES] for v in range(width // LANES)]
            lists += [jnp.where(slot < len_ref[i], cand_ref[i : i + 1, :], -1).astype(F32), dead]
        for i in range(0, share, 2):
            parts.append(jnp.concatenate(lists[2 * i : 2 * i + 4], axis=1))
    block = jnp.concatenate(parts, axis=0)
    rows = block.shape[0]
    for p in range(out_ref.shape[0] // rows):
        out_ref[p * rows : (p + 1) * rows, :] = block


def unpack(word):
    blocks = []
    for h in range(2):
        half = lax.shift_right_logical(word, 16 * h).astype(I16)
        planes = []
        for k in range(16):
            bit = jnp.int16(-(2**15) if k == 15 else 1 << k)
            planes.append(jnp.where((half & bit) != 0, BF16(1), BF16(-1)))
        blocks.append(jnp.concatenate(planes, axis=0).astype(F8))
    return blocks


def main_kernel(share, group, cols, edges_ref, x_ref, codes_ref, quant_ref, scale_ref, out_ref, signs_s, qhl_s, bits_s, place_s):
    count, width = quant_ref.shape
    vregs = width // LANES
    rows = share * vregs + share // 2
    sources = x_ref.shape[0] // rows
    nq = group * share
    nbins = edges_ref.shape[1] - 1
    src = lax.broadcasted_iota(I32, (2 * TILE, TILE), 0)
    dst = lax.broadcasted_iota(I32, (2 * TILE, TILE), 1)
    perms = [jnp.where(src == (dst & 15) * 32 + 16 * h + (dst >> 4), 1.0, 0.0).astype(BF16) for h in range(2)]
    lane = lax.broadcasted_iota(I32, (LANES, LANES), 1)
    for k in range(nbins):
        place_s[k * LANES : (k + 1) * LANES, :] = jnp.where(lane == LANES // 2 + k, 1.0, 0.0).astype(BF16)
    edge = [jnp.broadcast_to(edges_ref[:, k : k + 1], (8, LANES)) for k in range(nbins + 1)]
    dist = lax.broadcasted_iota(I32, (8, LANES), 1) + edge[0] - 1
    tables = []
    for j in range(-(-nbins // 4)):
        word = jnp.zeros((8, LANES), I32)
        for k in range(4 * j, min(4 * j + 4, nbins)):
            inside = (dist >= edge[k]) & (dist < edge[k + 1])
            word = word + jnp.where(inside, jnp.int32(1 << (8 * (k - 4 * j))), 0)
        tables.append(jnp.concatenate([word] * (nq // 8), axis=0))
    offset = jnp.concatenate([(width // 2 + 1 - edge[0]).astype(F32)] * (nq // 8), axis=0)

    def serve(start):
        lane = lax.broadcasted_iota(I32, (group, LANES), 1)
        full, index = [], []
        for i in range(share):
            at = start * rows + i * vregs
            full.append(jnp.concatenate([x_ref[pl.ds(at + v, group, stride=rows), :] for v in range(vregs)], axis=1))
            got = x_ref[pl.ds(start * rows + share * vregs + i // 2, group, stride=rows), :]
            if i % 2:
                got = pltpu.roll(got, LANES // 2, 1)
            index.append(jnp.where(lane < LANES // 2, got, -1.0).astype(I32))
        full = jnp.concatenate(full, axis=0)
        index = jnp.concatenate(index, axis=0)
        index = jnp.where(index < 0, -1, index - lax.axis_index("corpus") * count)
        low = index & (LANES - 1)
        high = index >> 7
        hi = full.astype(BF16)
        qhl_s[:nq, :] = hi
        qhl_s[nq:, :] = (full - hi.astype(F32)).astype(BF16)
        signs = jnp.where(full >= 0, -0.5, 0.5).astype(BF16)
        for h in range(2):
            for b in range(width // (2 * TILE)):
                at = (2 * b + h) * TILE
                signs_s[:, at : at + TILE] = jnp.dot(
                    signs[:, 2 * b * TILE : (2 * b + 2) * TILE], perms[h], preferred_element_type=F32
                ).astype(F8)

        tally = [jnp.zeros((nq, LANES), I32) for _ in tables]
        scores = jnp.zeros((nq, LANES), F32)
        for i in range(count // cols):
            at = slice(i * cols, (i + 1) * cols)
            for b in range(width // (2 * TILE)):
                for h, block in enumerate(unpack(codes_ref[16 * b : 16 * b + 16, at])):
                    bits_s[(2 * b + h) * TILE : (2 * b + h + 1) * TILE, at] = block
            half = jnp.dot(signs_s[...], bits_s[:, at], preferred_element_type=F32)
            prod = lax.dot_general(
                qhl_s[...], quant_ref[at, :], (((1,), (1,)), ((), ())), preferred_element_type=F32
            )
            for j in range(cols // LANES):
                cut = slice(j * LANES, (j + 1) * LANES)
                where = jnp.clip(half[:, cut] + offset, 0.0, LANES - 1.0).astype(I32)
                tally = [
                    t + jnp.take_along_axis(w, where, axis=1, mode="promise_in_bounds") for t, w in zip(tally, tables)
                ]
                row = i * (cols // LANES) + j
                value = (prod[:nq, cut] + prod[nq:, cut]) * scale_ref[:, row * LANES : (row + 1) * LANES]
                value = jnp.take_along_axis(value, low, axis=1, mode="promise_in_bounds")
                scores = jnp.where(high == row, value, scores)
        planes = [((tally[k // 4] >> (8 * (k % 4))) & 255).astype(F32).astype(BF16) for k in range(nbins)]
        counts = jnp.dot(jnp.concatenate(planes, axis=1), place_s[...], preferred_element_type=F32)
        lane = lax.broadcasted_iota(I32, (nq, LANES), 1)
        res = jnp.where(lane < LANES // 2, scores, counts)
        for i in range(share):
            out_ref[pl.ds(start * share + i, group, stride=share), :] = res[i * group : (i + 1) * group, :]

    if sources == group:
        serve(0)
    else:
        pl.loop(0, sources // group)(lambda g: serve(g * group))


def shards(chips, cores, queries, codes, quant_rows, row_scale, candidates, shortlist, edges):
    both = ("corpus", "batch")
    own, width = queries.shape
    slots = candidates.shape[1]
    count, words = codes.shape
    nbins = edges.shape[0] - 1
    devices = chips * cores
    share = own // cores
    nq = share * devices
    cols = 768 if count % 768 == 0 else 512
    group = math.gcd(devices, 32)
    part = group * share
    rows = share * (width // LANES) + share // 2
    assert own % (2 * cores) == 0
    assert words % 16 == 0 and width == 32 * words and count % 512 == 0
    assert count // LANES < 256 and slots <= LANES // 2 and nbins <= LANES // 2
    payload = pl.pallas_call(
        functools.partial(pack_kernel, share),
        in_specs=[VMEM, VMEM, SMEM],
        out_specs=VMEM,
        out_shape=pltpu.VMEM((devices * rows, LANES), F32),
        compiler_params=pltpu.CompilerParams(vmem_limit_bytes=2 << 20),
        name="pack",
    )(far(queries), far(candidates), far(shortlist))
    payload = pl.pallas_call(
        lambda x_ref, out_ref: None,
        in_specs=[VMEM],
        out_specs=VMEM,
        out_shape=pltpu.VMEM((devices * rows, LANES), F32),
        input_output_aliases={0: 0},
        compiler_params=pltpu.CompilerParams(vmem_limit_bytes=1 << 20),
        cost_estimate=pl.CostEstimate(flops=10**10, bytes_accessed=0, transcendentals=0),
        name="gate",
    )(near(payload))
    got = lax.all_to_all(payload.reshape(devices, 1, rows * LANES), both, 0, 0).reshape(devices * rows, LANES)
    result = pl.pallas_call(
        functools.partial(main_kernel, share, group, cols),
        in_specs=[VMEM, VMEM, VMEM, VMEM, VMEM],
        out_specs=VMEM,
        out_shape=pltpu.VMEM((nq, LANES), F32),
        scratch_shapes=[
            pltpu.VMEM((part, width), F8),
            pltpu.VMEM((2 * part, width), BF16),
            pltpu.VMEM((width, count), F8),
            pltpu.VMEM((nbins * LANES, LANES), BF16),
        ],
        compiler_params=pltpu.CompilerParams(vmem_limit_bytes=24 << 20),
        cost_estimate=pl.CostEstimate(flops=4 * 10**9, bytes_accessed=0, transcendentals=0),
        name="main",
    )(near(edges.reshape(1, nbins + 1)), near(got), codes.T, quant_rows, row_scale.reshape(1, count))
    back = lax.all_to_all(result.reshape(devices, 1, share * LANES), both, 0, 0)
    total = jnp.sum(back.reshape(chips, own, LANES), axis=0)
    hist = total[:, LANES // 2 : LANES // 2 + nbins] * (nbins / (count * chips))
    return hist, total[:, :slots]


def solution(mesh):
    both = ("corpus", "batch")
    return jax.shard_map(
        functools.partial(shards, mesh.shape["corpus"], mesh.shape["batch"]),
        mesh=mesh,
        in_specs=(P(both, None), P("corpus", None), P("corpus", None), P("corpus"), P(both, None), P(both), P()),
        out_specs=(P(both, None), P(both, None)),
        check_vma=False,
    )
```

```python
import functools
import math

import jax
import jax.numpy as jnp
from jax import lax
from jax.experimental import pallas as pl
from jax.experimental.pallas import tpu as pltpu
from jax.sharding import PartitionSpec as P

LANES = 128
TILE = 256
F32, BF16, I32, I16, F8 = jnp.float32, jnp.bfloat16, jnp.int32, jnp.int16, jnp.float8_e4m3fn
VMEM = pl.BlockSpec(memory_space=pltpu.VMEM)
SMEM = pl.BlockSpec(memory_space=pltpu.SMEM)
ANY = pl.BlockSpec(memory_space=pl.ANY)


def near(x):
    return pltpu.with_memory_space_constraint(x, pltpu.VMEM)


def far(x):
    return pltpu.with_memory_space_constraint(x, pltpu.HBM)


def pack_kernel(share, q_ref, cand_ref, len_ref, out_ref):
    own, width = q_ref.shape
    slots = cand_ref.shape[1]
    slot = lax.broadcasted_iota(I32, (1, slots), 1)
    dead = jnp.full((1, LANES // 2 - slots), -1.0, F32)
    parts = []
    for first in range(0, own, share):
        lists = []
        for i in range(first, first + share):
            parts += [q_ref[i : i + 1, v * LANES : (v + 1) * LANES] for v in range(width // LANES)]
            lists += [jnp.where(slot < len_ref[i], cand_ref[i : i + 1, :], -1).astype(F32), dead]
        for i in range(0, share, 2):
            parts.append(jnp.concatenate(lists[2 * i : 2 * i + 4], axis=1))
    block = jnp.concatenate(parts, axis=0)
    rows = block.shape[0]
    for p in range(out_ref.shape[0] // rows):
        out_ref[p * rows : (p + 1) * rows, :] = block


def unpack(word):
    blocks = []
    for h in range(2):
        half = lax.shift_right_logical(word, 16 * h).astype(I16)
        planes = []
        for k in range(16):
            bit = jnp.int16(-(2**15) if k == 15 else 1 << k)
            planes.append(jnp.where((half & bit) != 0, BF16(1), BF16(-1)))
        blocks.append(jnp.concatenate(planes, axis=0).astype(F8))
    return blocks


def main_kernel(share, group, cols, edges_ref, x_ref, codes_ref, quant_ref, scale_ref, out_ref, signs_s, qhl_s, bits_s, place_s):
    count, width = quant_ref.shape
    vregs = width // LANES
    rows = share * vregs + share // 2
    sources = x_ref.shape[0] // rows
    nq = group * share
    nbins = edges_ref.shape[1] - 1
    src = lax.broadcasted_iota(I32, (2 * TILE, TILE), 0)
    dst = lax.broadcasted_iota(I32, (2 * TILE, TILE), 1)
    perms = [jnp.where(src == (dst & 15) * 32 + 16 * h + (dst >> 4), 1.0, 0.0).astype(BF16) for h in range(2)]
    lane = lax.broadcasted_iota(I32, (LANES, LANES), 1)
    for k in range(nbins):
        place_s[k * LANES : (k + 1) * LANES, :] = jnp.where(lane == LANES // 2 + k, 1.0, 0.0).astype(BF16)
    edge = [jnp.broadcast_to(edges_ref[:, k : k + 1], (8, LANES)) for k in range(nbins + 1)]
    dist = lax.broadcasted_iota(I32, (8, LANES), 1) + edge[0] - 1
    tables = []
    for j in range(-(-nbins // 4)):
        word = jnp.zeros((8, LANES), I32)
        for k in range(4 * j, min(4 * j + 4, nbins)):
            inside = (dist >= edge[k]) & (dist < edge[k + 1])
            word = word + jnp.where(inside, jnp.int32(1 << (8 * (k - 4 * j))), 0)
        tables.append(jnp.concatenate([word] * (nq // 8), axis=0))
    offset = jnp.concatenate([(width // 2 + 1 - edge[0]).astype(F32)] * (nq // 8), axis=0)

    def serve(start):
        lane = lax.broadcasted_iota(I32, (group, LANES), 1)
        full, index = [], []
        for i in range(share):
            at = start * rows + i * vregs
            full.append(jnp.concatenate([x_ref[pl.ds(at + v, group, stride=rows), :] for v in range(vregs)], axis=1))
            got = x_ref[pl.ds(start * rows + share * vregs + i // 2, group, stride=rows), :]
            if i % 2:
                got = pltpu.roll(got, LANES // 2, 1)
            index.append(jnp.where(lane < LANES // 2, got, -1.0).astype(I32))
        full = jnp.concatenate(full, axis=0)
        index = jnp.concatenate(index, axis=0)
        index = jnp.where(index < 0, -1, index - lax.axis_index("corpus") * count)
        low = index & (LANES - 1)
        high = index >> 7
        hi = full.astype(BF16)
        qhl_s[:nq, :] = hi
        qhl_s[nq:, :] = (full - hi.astype(F32)).astype(BF16)
        signs = jnp.where(full >= 0, -0.5, 0.5).astype(BF16)
        for h in range(2):
            for b in range(width // (2 * TILE)):
                at = (2 * b + h) * TILE
                signs_s[:, at : at + TILE] = jnp.dot(
                    signs[:, 2 * b * TILE : (2 * b + 2) * TILE], perms[h], preferred_element_type=F32
                ).astype(F8)

        tally = [jnp.zeros((nq, LANES), I32) for _ in tables]
        scores = jnp.zeros((nq, LANES), F32)
        for i in range(count // cols):
            at = slice(i * cols, (i + 1) * cols)
            for b in range(width // (2 * TILE)):
                for h, block in enumerate(unpack(codes_ref[16 * b : 16 * b + 16, at])):
                    bits_s[(2 * b + h) * TILE : (2 * b + h + 1) * TILE, at] = block
            half = jnp.dot(signs_s[...], bits_s[:, at], preferred_element_type=F32)
            prod = lax.dot_general(
                qhl_s[...], quant_ref[at, :], (((1,), (1,)), ((), ())), preferred_element_type=F32
            )
            for j in range(cols // LANES):
                cut = slice(j * LANES, (j + 1) * LANES)
                where = jnp.clip(half[:, cut] + offset, 0.0, LANES - 1.0).astype(I32)
                tally = [
                    t + jnp.take_along_axis(w, where, axis=1, mode="promise_in_bounds") for t, w in zip(tally, tables)
                ]
                row = i * (cols // LANES) + j
                value = (prod[:nq, cut] + prod[nq:, cut]) * scale_ref[:, row * LANES : (row + 1) * LANES]
                value = jnp.take_along_axis(value, low, axis=1, mode="promise_in_bounds")
                scores = jnp.where(high == row, value, scores)
        planes = [((tally[k // 4] >> (8 * (k % 4))) & 255).astype(F32).astype(BF16) for k in range(nbins)]
        counts = jnp.dot(jnp.concatenate(planes, axis=1), place_s[...], preferred_element_type=F32)
        lane = lax.broadcasted_iota(I32, (nq, LANES), 1)
        res = jnp.where(lane < LANES // 2, scores, counts)
        for i in range(share):
            out_ref[pl.ds(start * share + i, group, stride=share), :] = res[i * group : (i + 1) * group, :]

    if sources == group:
        serve(0)
    else:
        pl.loop(0, sources // group)(lambda g: serve(g * group))


def finish_kernel(unit, back_ref, hist_ref, scores_ref):
    own, nbins = hist_ref.shape
    total = jnp.zeros((own, LANES), F32)
    for c in range(back_ref.shape[0] // own):
        total = total + back_ref[c * own : (c + 1) * own, :]
    hist_ref[...] = total[:, LANES // 2 : LANES // 2 + nbins] * unit
    scores_ref[...] = total[:, : scores_ref.shape[1]]


def shards(chips, cores, queries, codes, quant_rows, row_scale, candidates, shortlist, edges):
    both = ("corpus", "batch")
    own, width = queries.shape
    slots = candidates.shape[1]
    count, words = codes.shape
    nbins = edges.shape[0] - 1
    devices = chips * cores
    share = own // cores
    nq = share * devices
    cols = 768 if count % 768 == 0 else 512
    group = math.gcd(devices, 32)
    part = group * share
    rows = share * (width // LANES) + share // 2
    assert own % (2 * cores) == 0
    assert words % 16 == 0 and width == 32 * words and count % 512 == 0
    assert count // LANES < 256 and slots <= LANES // 2 and nbins <= LANES // 2
    payload = pl.pallas_call(
        functools.partial(pack_kernel, share),
        in_specs=[VMEM, VMEM, SMEM],
        out_specs=VMEM,
        out_shape=pltpu.VMEM((devices * rows, LANES), F32),
        compiler_params=pltpu.CompilerParams(vmem_limit_bytes=2 << 20),
        cost_estimate=pl.CostEstimate(flops=10**10, bytes_accessed=0, transcendentals=0),
        name="pack",
    )(far(queries), far(candidates), far(shortlist))
    got = lax.all_to_all(payload.reshape(devices, 1, rows * LANES), both, 0, 0).reshape(devices * rows, LANES)
    result = pl.pallas_call(
        functools.partial(main_kernel, share, group, cols),
        in_specs=[VMEM, VMEM, VMEM, VMEM, VMEM],
        out_specs=VMEM,
        out_shape=pltpu.VMEM((nq, LANES), F32),
        scratch_shapes=[
            pltpu.VMEM((part, width), F8),
            pltpu.VMEM((2 * part, width), BF16),
            pltpu.VMEM((width, count), F8),
            pltpu.VMEM((nbins * LANES, LANES), BF16),
        ],
        compiler_params=pltpu.CompilerParams(vmem_limit_bytes=24 << 20),
        cost_estimate=pl.CostEstimate(flops=4 * 10**9, bytes_accessed=0, transcendentals=0),
        name="main",
    )(near(edges.reshape(1, nbins + 1)), near(got), codes.T, quant_rows, row_scale.reshape(1, count))
    back = lax.all_to_all(result.reshape(devices, 1, share * LANES), both, 0, 0)
    return pl.pallas_call(
        functools.partial(finish_kernel, nbins / (count * chips)),
        in_specs=[VMEM],
        out_specs=[VMEM, VMEM],
        out_shape=[jax.ShapeDtypeStruct((own, nbins), F32), jax.ShapeDtypeStruct((own, slots), F32)],
        name="finish",
    )(near(back.reshape(nq, LANES)))


def solution(mesh):
    both = ("corpus", "batch")
    return jax.shard_map(
        functools.partial(shards, mesh.shape["corpus"], mesh.shape["batch"]),
        mesh=mesh,
        in_specs=(P(both, None), P("corpus", None), P("corpus", None), P("corpus"), P(both, None), P(both), P()),
        out_specs=(P(both, None), P(both, None)),
        check_vma=False,
    )
```
